32 devices in a mesh: blk: 8 (over y, x, core), uly: 4 (over z).
Axes of the slice: x: 2, y: 2, z: 4, core: 2. Of those that a mesh axis runs over, the one named last changes fastest.
Arguments:
- self_query: bfloat16 [1280, 5120], P(('blk', 'uly')), may hold values from -8 to 8
- self_key: bfloat16 [1280, 5120], P(('blk', 'uly')), may hold values from -8 to 8
- self_value: bfloat16 [1280, 5120], P(('blk', 'uly')), may hold values from -6 to 6
- cross_query: bfloat16 [1280, 5120], P(('blk', 'uly')), may hold values from -8 to 8
- text_key: bfloat16 [512, 5120], P('blk', 'uly'), may hold values from -8 to 8
- text_value: bfloat16 [512, 5120], P('blk', 'uly'), may hold values from -6 to 6
- padded_count: int32 [1], replicated, may hold values from 0 to 320
Outputs:
- self_out: bfloat16 [1280, 5120], P(('blk', 'uly'))
- cross_out: bfloat16 [1280, 5120], P(('blk', 'uly'))
The draws below stay inside these ranges and needn't reach their ends.
All inputs are finite; a program needn't handle non-finite values.
Results may differ from the reference program's by a relative error of at most 0.0099.
Values may be sent and summed in bfloat16 or wider, within the bound.
A program may use at most 128 MiB of HBM per device.

```python
import math
import jax
import jax.numpy as jnp
from jax import lax

HEADS = 40
HD = 128
TEXT = 512
TH = 4
TW = 10
ROW_TILES = 8
FRAMES = 1
GRID_H = 32
GRID_W = 40
TOKENS = 1280
N_ULY = 4


def draw_self_query(key, part):
    own_key = jax.random.fold_in(key, 1)
    values = 1.8 * jax.random.truncated_normal(own_key, -4.0, 4.0, (TOKENS, HEADS * HD), jnp.float32)
    return values.astype(jnp.bfloat16)


def draw_self_key(key, part):
    own_key = jax.random.fold_in(key, 2)
    values = 1.8 * jax.random.truncated_normal(own_key, -4.0, 4.0, (TOKENS, HEADS * HD), jnp.float32)
    return values.astype(jnp.bfloat16)


def draw_cross_query(key, part):
    own_key = jax.random.fold_in(key, 3)
    values = 1.6 * jax.random.truncated_normal(own_key, -4.0, 4.0, (TOKENS, HEADS * HD), jnp.float32)
    return values.astype(jnp.bfloat16)


def draw_text_key(key, part):
    own_key = jax.random.fold_in(key, 4)
    values = 1.6 * jax.random.truncated_normal(own_key, -4.0, 4.0, (TEXT, HEADS * HD), jnp.float32)
    return values.astype(jnp.bfloat16)


def shard_levels(key, dims, cuts, smallest, top_value):
    gain, own = 1.0, jax.random.fold_in(key, 6)
    for dim, blocks in cuts:
        heights = jnp.exp(jax.random.uniform(jax.random.fold_in(own, dim), (blocks,), jnp.float32, smallest / len(cuts), top_value / len(cuts)))
        gain = gain * jnp.repeat(heights, dims[dim] // blocks).reshape([-1 if axis == dim else 1 for axis in range(len(dims))])
    return gain


def centred(key, shape, scale, reach, cuts=(), kind=jnp.bfloat16):
    values = scale * jax.random.normal(key, shape, jnp.float32)
    if cuts:
        values = values * shard_levels(key, shape, cuts, -0.22, 0.18)
    return jnp.clip(values, -reach, reach).astype(kind)


def setup_inputs(seed: int = 0) -> dict:
    keys = jax.random.split(jax.random.key(seed), 8)
    return {
        "self_query": draw_self_query(jax.random.fold_in(keys[7], 71), 0),
        "self_key": draw_self_key(jax.random.fold_in(keys[7], 71), 0),
        "self_value": centred(keys[2], (TOKENS, HEADS * HD), 1.0, 6.0, ((0, 32),)),
        "cross_query": draw_cross_query(jax.random.fold_in(keys[7], 71), 0),
        "text_key": draw_text_key(jax.random.fold_in(keys[7], 71), 0),
        "text_value": centred(keys[5], (TEXT, HEADS * HD), 1.0, 6.0, ((0, 8), (1, 4))),
        "padded_count": jax.random.randint(keys[6], (1,), 0, TOKENS // 4 + 1).astype(jnp.int32),
    }


neg_fill = -1e+30

def rope_tables(raster, head_size, grid_height, grid_width):
    frame_cells = grid_height * grid_width
    frame_index = raster // frame_cells
    row_index = raster // grid_width % grid_height
    col_index = raster % grid_width
    pair_index = lax.iota(jnp.int32, head_size) // 2
    side_pairs = head_size // 6
    first_pairs = head_size // 2 - 2 * side_pairs
    in_frames = pair_index < first_pairs
    in_rows = pair_index < first_pairs + side_pairs
    numerator = jnp.where(in_frames, pair_index, jnp.where(in_rows, pair_index - first_pairs, pair_index - first_pairs - side_pairs)).astype(jnp.float32)
    denominator = jnp.where(in_frames, first_pairs, side_pairs).astype(jnp.float32)
    omegas = jnp.power(jnp.float32(10000.0), -(numerator / denominator))
    position = jnp.where(in_frames[None, :], frame_index[:, None], jnp.where(in_rows[None, :], row_index[:, None], col_index[:, None])).astype(jnp.float32)
    angles = position * omegas[None, :]
    return (jnp.cos(angles), jnp.sin(angles))

def rotate(values, cosine_table, sine_table):
    channels = values.shape[1]
    repeats = channels // cosine_table.shape[1]
    widened = values.astype(jnp.float32)
    channel = lax.iota(jnp.int32, channels)
    partner = jnp.where(channel % 2 == 0, -jnp.roll(widened, -1, axis=1), jnp.roll(widened, 1, axis=1))
    return (widened * jnp.tile(cosine_table, (1, repeats)) + partner * jnp.tile(sine_table, (1, repeats))).astype(jnp.bfloat16)

def softmax_rows(query_block, key_rows, value_rows, key_mask, scaling):
    scores = jnp.dot(query_block, key_rows.T, preferred_element_type=jnp.float32) * scaling
    if key_mask is not None:
        scores = jnp.where(key_mask[None, :], scores, neg_fill)
    row_peak = lax.optimization_barrier(jnp.max(scores, axis=1, keepdims=True))
    weights = jnp.exp(scores - row_peak)
    totals = lax.optimization_barrier(jnp.sum(weights, axis=1, keepdims=True))
    weighted = jnp.dot(weights.astype(jnp.bfloat16), value_rows, preferred_element_type=jnp.float32)
    return (weighted / totals).astype(jnp.bfloat16)

def attention(queries, keys_all, values_all, key_mask, scaling):
    query_count = queries.shape[0]
    block_rows = 512 if query_count % 512 == 0 else query_count
    block_count = query_count // block_rows
    query_heads = queries.reshape(block_count, block_rows, HEADS, HD).transpose(2, 0, 1, 3)
    key_heads = keys_all.reshape(keys_all.shape[0], HEADS, HD).transpose(1, 0, 2)
    value_heads = values_all.reshape(values_all.shape[0], HEADS, HD).transpose(1, 0, 2)

    def one_head(head_index):

        def one_block(block_index):
            return softmax_rows(query_heads[head_index, block_index], key_heads[head_index], value_heads[head_index], key_mask, scaling)
        return lax.map(one_block, jnp.arange(block_count, dtype=jnp.int32))
    outputs = lax.map(one_head, jnp.arange(HEADS, dtype=jnp.int32))
    return outputs.transpose(1, 2, 0, 3).reshape(query_count, HEADS * HD)

def reference(self_query, self_key, self_value, cross_query, text_key, text_value, padded_count):
    channels = HEADS * HD

    def frame_major(array):
        tile_grid = array.reshape(FRAMES, ROW_TILES, N_ULY, TH, TW, channels)
        return tile_grid.transpose(0, 1, 3, 2, 4, 5).reshape(TOKENS, channels)
    query_rows = frame_major(self_query)
    key_rows = frame_major(self_key)
    value_rows = frame_major(self_value)
    cross_rows = frame_major(cross_query)
    raster = lax.iota(jnp.int32, TOKENS)
    cosine_table, sine_table = rope_tables(raster, HD, GRID_H, GRID_W)
    query_rot = rotate(query_rows, cosine_table, sine_table)
    key_rot = rotate(key_rows, cosine_table, sine_table)
    scaling = 1.0 / math.sqrt(HD)
    key_mask = raster < TOKENS - padded_count[0]
    self_out = attention(query_rot, key_rot, value_rows, key_mask, scaling)
    cross_out = attention(cross_rows, text_key, text_value, None, scaling)
    return (self_out, cross_out)
```

```python
import functools
import math

import jax
import jax.numpy as jnp
import numpy as np
from jax import lax
from jax.experimental import pallas as pl
from jax.experimental.pallas import tpu as pltpu
from jax.sharding import PartitionSpec as P

HD = 128
TH = 4
TW = 10
ROW_TILES = 8

MESH = pl.DeviceIdType.MESH
neg_fill = -1e30
KEY_BLOCK = 1280
VALUE_CUT = (1, 2, 2)
KEY_CUT = (1, 2, 2)
CROSS_CUT = (1, 4)
QUERY_CUT = (5,)
CROSS_BACK = (1,)
SELF_BACK = (2, 3)


def pieces(heads, sizes):
    cuts, start, index = [], 0, 0
    while start < heads:
        stop = min(heads, start + sizes[min(index, len(sizes) - 1)])
        cuts.append((start, stop))
        start, index = stop, index + 1
    return cuts


def rope_parts(blocks, groups):
    grid_height, grid_width = TH * ROW_TILES, TW * groups
    side = HD // 6
    first = HD // 2 - 2 * side
    pair = np.arange(HD) // 2
    start = np.where(pair < first, 0, np.where(pair < first + side, first, first + side))
    power = -((pair - start) / np.where(pair < first, first, side))
    omegas = np.power(10000.0, power).astype(np.float32)
    i, j = (axis.reshape(-1) for axis in np.meshgrid(np.arange(TH), np.arange(TW), indexing="ij"))
    rows = np.arange(blocks)[:, None] * TH + i[None, :]
    cols = np.arange(groups)[:, None] * TW + j[None, :]
    by_block = np.where(
        pair < first, (rows // grid_height)[..., None], (rows % grid_height)[..., None]
    )
    is_col = pair >= first + side

    def table(position, mine):
        angles = position.astype(np.float32) * omegas
        parts = [np.where(mine, np.cos(angles), 0), np.where(mine, np.sin(angles), 0)]
        return np.concatenate(parts, axis=-1).astype(np.float32)

    return table(by_block, ~is_col), table(np.broadcast_to(cols[..., None], cols.shape + (HD,)), is_col)


def dot(a, b):
    return jnp.dot(a, b, preferred_element_type=jnp.float32)


def dot_t(a, b):
    return lax.dot_general(a, b, (((1,), (1,)), ((), ())), preferred_element_type=jnp.float32)


def attend(queries, key_ref, value_ref, cols, bias_ref, factor):
    rows = key_ref.shape[0]
    step = rows if rows <= 2 * KEY_BLOCK else KEY_BLOCK

    def scores_of(start):
        s = dot_t(queries, key_ref[pl.ds(start, step), cols]) * factor
        if bias_ref is not None:
            s = s + bias_ref[:, pl.ds(start, step)]
        return s

    if step == rows:
        s = scores_of(0)
        w = jnp.exp2(s - jnp.max(s, axis=1, keepdims=True))
        total = jnp.sum(w, axis=1, keepdims=True)
        out = dot(w.astype(jnp.bfloat16), value_ref[:, cols])
        return (out / total).astype(jnp.bfloat16)

    def advance(index, state):
        peak, total, out = state
        start = pl.multiple_of(index * step, step)
        s = scores_of(start)
        new_peak = jnp.maximum(peak, jnp.max(s, axis=1, keepdims=True))
        w = jnp.exp2(s - new_peak)
        shrink = jnp.exp2(peak - new_peak)
        total = total * shrink + jnp.sum(w, axis=1, keepdims=True)
        out = out * shrink + dot(w.astype(jnp.bfloat16), value_ref[pl.ds(start, step), cols])
        return new_peak, total, out

    m = queries.shape[0]
    state = (
        jnp.full((m, 1), neg_fill, jnp.float32),
        jnp.zeros((m, 1), jnp.float32),
        jnp.zeros((m, HD), jnp.float32),
    )
    peak, total, out = lax.fori_loop(0, rows // step, advance, state)
    return (out / total).astype(jnp.bfloat16)


def kernel(cfg, pad_ref, q_hbm, k_hbm, v_hbm, c_ref, tk_ref, tv_ref, rope_blk, rope_col, spin_hbm,
           perm_hbm, pos_hbm, so_ref, co_ref, spin_ref, perm_ref, pos_ref, v_raw, q_raw, k_raw, tab, q_src, k_src, kv_all, q_in, c_in, text_all,
           s_out, c_out, bias, in_sem, g_recv, t_in, tg_recv, o_recv, sent, load, ready):
    U, pair, N, heads = cfg
    tokens = v_hbm.shape[0]
    width = heads * HD
    groups = U * pair
    blk = lax.axis_index("blk")
    z = lax.axis_index("uly")
    n = blk // pair
    core = blk % pair
    me = z * pair + core
    slot = (core * U + z) * tokens
    shard = groups * tokens
    text_rows = tk_ref.shape[0]
    text_shard = pair * text_rows
    bits = int(math.log2(N))
    staged = U == 4 and pair == 2
    factor = math.log2(math.e) / math.sqrt(HD)

    def apart(dz):
        if U & (U - 1):
            return (z + dz) % U
        out = 0
        for bit in range(U.bit_length() - 1):
            mine = (z // (1 << bit)) % 2
            out = out + (1 - mine if (dz >> bit) & 1 else mine) * (1 << bit)
        return out

    far_first = [*range(U // 2, U), *range(1, U // 2), 0] if U > 1 else [0]
    offsets = [(dz, dc) for dz in far_first for dc in reversed(range(pair))]

    def group_device(d):
        dz, dc = offsets[d - 1]
        to_z, to_core = apart(dz), (core + dc) % pair
        return to_z * pair + to_core, (n * pair + to_core, to_z)

    def flip(index, bit):
        return index + (1 - 2 * ((index // (1 << bit)) % 2)) * (1 << bit)

    def neighbour(bit):
        return (flip(n, bit) * pair + core, z)

    def fetch(index, src, dst):
        copy = pltpu.make_async_copy(src, dst, load.at[index])
        copy.start()
        return copy

    v_load, k_load = fetch(0, v_hbm, v_raw), fetch(1, k_hbm, k_raw)
    fetch(2, rope_blk.at[blk], tab.at[0])
    fetch(2, rope_col.at[z], tab.at[1])
    spin_load = fetch(3, spin_hbm, spin_ref)

    k_all, v_all = kv_all.at[0], kv_all.at[1]
    tk_all, tv_all = text_all.at[0], text_all.at[1]

    barrier = pltpu.get_barrier_semaphore()
    partner = (n * pair + (core + 1) % pair, z)
    inner = (z > 0) & (z < U - 1)
    across = (blk, U - 1 - z)

    def greet(sem, device):
        pl.semaphore_signal(sem, inc=1, device_id=device, device_id_type=MESH)

    if staged:
        greet(barrier, partner)

        @pl.when((core == 0) & inner)
        def _():
            greet(barrier, across)
            pl.semaphore_wait(barrier, 2)

        @pl.when((core == 0) & jnp.logical_not(inner))
        def _():
            pl.semaphore_wait(barrier, 1)

        @pl.when(core == 1)
        def _():
            for b in range(bits):
                greet(barrier, neighbour(b))

            @pl.when(z > 0)
            def _():
                greet(barrier, (blk, z - 1))

            @pl.when(z < U - 1)
            def _():
                greet(barrier, (blk, z + 1))

            @pl.when(inner)
            def _():
                pl.semaphore_wait(barrier, 3 + bits)

            @pl.when(jnp.logical_not(inner))
            def _():
                pl.semaphore_wait(barrier, 2 + bits)
    else:
        peers = [group_device(d)[1] for d in range(1, groups)] + [neighbour(b) for b in range(bits)]
        for peer in peers:
            greet(barrier, peer)
        pl.semaphore_wait(barrier, len(peers))

    def remote(src, dst, kind, recv, device):
        pltpu.make_async_remote_copy(
            src_ref=src, dst_ref=dst, send_sem=sent.at[kind], recv_sem=recv, device_id=device,
            device_id_type=MESH,
        ).start()

    def wait(ref, sem):
        pltpu.make_async_copy(ref, ref, sem).wait()

    def head_cols(h):
        return pl.ds(h * HD, HD)

    def span(piece):
        return pl.ds(piece[0] * HD, (piece[1] - piece[0]) * HD)

    def scatter_one(src, place, sem, piece, e, device):
        cols = (piece[1] - piece[0]) * HD
        block = src.at[:, pl.ds(pl.multiple_of(e * width + piece[0] * HD, HD), cols)]
        if device is None:
            pltpu.make_async_copy(block, place, sem).start()
        else:
            remote(block, place, 0, sem, device)

    def scatter(src, dst, base, sems, cuts, early=False):
        for index, piece in enumerate(cuts):
            place = dst.at[pl.ds(pl.multiple_of(base + slot, 8), tokens), span(piece)]
            for d in range(1, groups + 1):
                e, device = group_device(d)
                if d == groups:
                    scatter_one(src, place, in_sem.at[sems + index], piece, e, None)
                elif early and offsets[d - 1] == (U - 1, 0):

                    @pl.when(jnp.logical_not(inner))
                    def _():
                        scatter_one(src, place, in_sem.at[sems + index], piece, e, device)
                else:
                    scatter_one(src, place, in_sem.at[sems + index], piece, e, device)

    def scatter_early(src, dst, base, sems, cuts):
        @pl.when(inner)
        def _():
            for index, piece in enumerate(cuts):
                place = dst.at[pl.ds(pl.multiple_of(base + slot, 8), tokens), span(piece)]
                e = (U - 1 - z) * pair + core
                scatter_one(src, place, in_sem.at[sems + index], piece, e, across)

    v_cuts, k_cuts = pieces(heads, VALUE_CUT), pieces(heads, KEY_CUT)
    c_cuts, q_cuts = pieces(heads, CROSS_CUT), pieces(heads, QUERY_CUT)
    v_sems = 0
    k_sems = v_sems + len(v_cuts)
    c_sems = k_sems + len(k_cuts)
    q_sems = c_sems + len(c_cuts)

    def gossip():
        low, high, side, far, go = (ready.at[index] for index in range(5))

        @pl.when(z > 0)
        def _():
            greet(high, (blk, z - 1))

        @pl.when(z < U - 1)
        def _():
            greet(low, (blk, z + 1))

        for b in range(bits):
            greet(side, neighbour(b))

        @pl.when(z == 1)
        def _():
            pl.semaphore_wait(low, 1)
            greet(far, (blk, 2))
            pl.semaphore_wait(high, 1)
            greet(far, (blk, 0))
            pl.semaphore_wait(far, 1)
            greet(far, (blk, 0))

        @pl.when(z == 2)
        def _():
            pl.semaphore_wait(low, 1)
            greet(far, (blk, 3))
            pl.semaphore_wait(high, 1)
            greet(far, (blk, 1))
            pl.semaphore_wait(far, 1)
            greet(far, (blk, 3))

        @pl.when(z == 0)
        def _():
            pl.semaphore_wait(high, 1)
            pl.semaphore_wait(far, 2)

        @pl.when(z == 3)
        def _():
            pl.semaphore_wait(low, 1)
            pl.semaphore_wait(far, 2)

        pl.semaphore_wait(side, bits)
        greet(go, partner)

    def shard_at(ref, index, rows, cols):
        return ref.at[pl.ds(pl.multiple_of(index * rows, 8), rows), cols]

    def held(order, stage):
        lists = [[n]]
        for s in range(stage):
            lists.append([flip(i, order[s]) for part in lists for i in part])
        return lists

    def gather_send(ref, rows, cols, order, arrived, kind, recv_at):
        for stage in range(arrived, bits):
            device = neighbour(order[stage])
            for index in held(order, arrived)[arrived]:
                block = shard_at(ref, index, rows, cols)
                remote(block, block, kind, recv_at(stage), device)

    def gather_wait(ref, rows, cols, stage, recv_at):
        wait(ref.at[pl.ds(0, rows << stage), cols], recv_at(stage))

    orders = [list(range(bits)), list(range(bits))[::-1]]
    everything = pl.ds(0, width)

    def rope(src, dst):
        cos = tab[0, :, 0:HD] + tab[1, :, 0:HD]
        sin = tab[0, :, HD:] + tab[1, :, HD:]
        for g in range(src.shape[1] // HD):
            x = src[:, head_cols(g)]
            turned = x.astype(jnp.float32) * cos + dot(x, spin_ref[...]) * sin
            dst[:, head_cols(g)] = turned.astype(jnp.bfloat16)

    values_out = (v_raw, v_all, n * shard, v_sems, v_cuts)
    keys_out = (k_src, k_all, n * shard, k_sems, k_cuts)
    cross_out = (c_ref, c_in, 0, c_sems, c_cuts)
    v_load.wait()
    q_load = fetch(0, q_hbm, q_raw)
    if staged:
        scatter_early(*values_out)
        scatter_early(*cross_out)

        @pl.when(core == 1)
        def _():
            gossip()
            scatter(*values_out, True)

    k_load.wait()
    wait(tab, load.at[2])
    spin_load.wait()
    perm_load, pos_load = fetch(1, perm_hbm, perm_ref), fetch(3, pos_hbm, pos_ref)
    rope(k_raw, k_src)
    if staged:

        @pl.when(core == 0)
        def _():
            pl.semaphore_wait(ready.at[4], 1)
            scatter(*values_out, True)
    else:
        scatter(*values_out)

    text = ((tk_ref, tk_all, 0), (tv_ref, tv_all, 1))
    for src, dst, a in text:
        for d in range(pair):
            k = (core + d) % pair
            block = src.at[:, pl.ds(pl.multiple_of(k * width, HD), width)]
            place = dst.at[
                pl.ds(pl.multiple_of(n * text_shard + core * text_rows, 8), text_rows), everything
            ]
            if d == 0:
                pltpu.make_async_copy(block, place, t_in).start()
            else:
                remote(block, place, 2, t_in, (n * pair + k, z))

    scatter(*keys_out)
    scatter(*cross_out, staged)
    perm_load.wait()
    pos_load.wait()
    bias[...] = jnp.where(pos_ref[...] < k_all.shape[0] - pad_ref[0], 0.0, neg_fill)

    def text_recv(stage):
        return tg_recv.at[stage]

    def text_wait(stage):
        wait(text_all.at[:, pl.ds(0, text_shard << stage), :], tg_recv.at[stage])

    wait(text_all.at[:, pl.ds(0, text_shard), :], t_in)
    for _, dst, a in text:
        gather_send(dst, text_shard, everything, orders[a], 0, 2, text_recv)
    keys, values = (k_all, k_sems, 0, k_cuts), (v_all, v_sems, 1, v_cuts)

    def main_recv(sems, index):
        return lambda stage: g_recv.at[stage, sems + index]

    def own_sends(array, index):
        ref, sems, a, cuts = array
        cols = span(cuts[index])
        wait(shard_at(ref, n, shard, cols), in_sem.at[sems + index])
        gather_send(ref, shard, cols, orders[a], 0, 1, main_recv(sems, index))

    def relay(array, index):
        ref, sems, a, cuts = array
        cols = span(cuts[index])
        for stage in range(bits - 1):
            gather_wait(ref, shard, cols, stage, main_recv(sems, index))
            gather_send(ref, shard, cols, orders[a], stage + 1, 1, main_recv(sems, index))

    def settle(array, index):
        ref, sems, a, cuts = array
        if bits:
            gather_wait(ref, shard, span(cuts[index]), bits - 1, main_recv(sems, index))

    def opens(cuts, h):
        return [index for index, piece in enumerate(cuts) if piece[0] == h]

    def run_head(q_ref, key_ref, value_ref, bias_ref, out_ref, h):
        part = U * tokens

        for index in range(pair):
            rows = pl.ds(index * part, part)
            ordered = dot(perm_ref[...], q_ref[rows, head_cols(h)]).astype(jnp.bfloat16)
            out_ref[rows, head_cols(h)] = attend(
                ordered, key_ref, value_ref, head_cols(h), bias_ref, factor
            )

    def give_back(src, dst, recv, cuts, h):
        for piece in cuts:
            if piece[1] != h + 1:
                continue
            cols = (piece[1] - piece[0]) * HD
            for d in range(1, groups + 1):
                owner_core, owner_z = group_device(d)[1][0] % pair, group_device(d)[1][1]
                row = (owner_core * U + owner_z) * tokens
                block = src.at[pl.ds(pl.multiple_of(row, 8), tokens), span(piece)]
                place = dst.at[:, pl.ds(pl.multiple_of(me * width + piece[0] * HD, HD), cols)]
                if d == groups:
                    pltpu.make_async_copy(block, place, recv).start()
                else:
                    remote(block, place, 0, recv, (n * pair + owner_core, owner_z))

    for index in range(len(v_cuts)):
        own_sends(values, index)
    q_load.wait()
    rope(q_raw, q_src)
    scatter(q_src, q_in, 0, q_sems, q_cuts)
    for stage in range(bits - 1):
        text_wait(stage)
        for _, dst, a in text:
            gather_send(dst, text_shard, everything, orders[a], stage + 1, 2, text_recv)
    for index in range(len(k_cuts)):
        own_sends(keys, index)
        if 0 < index <= len(v_cuts):
            relay(values, index - 1)
    for index in range(len(k_cuts) - 1, len(v_cuts)):
        relay(values, index)
    if bits:
        text_wait(bits - 1)
    c_back, s_back = pieces(heads, CROSS_BACK), pieces(heads, SELF_BACK)
    for h in range(heads):
        for index in opens(k_cuts, h):
            relay(keys, index)
        for index in opens(c_cuts, h):
            wait(c_in.at[:, span(c_cuts[index])], in_sem.at[c_sems + index])
        run_head(c_in, tk_all, tv_all, None, c_out, h)
        give_back(c_out, co_ref, o_recv.at[1], c_back, h)
    for h in range(heads):
        for index in opens(q_cuts, h):
            wait(q_in.at[:, span(q_cuts[index])], in_sem.at[q_sems + index])
        for index in opens(v_cuts, h):
            settle(values, index)
        for index in opens(k_cuts, h):
            settle(keys, index)
        run_head(q_in, k_all, v_all, bias, s_out, h)
        give_back(s_out, so_ref, o_recv.at[0], s_back, h)

    own_rows = 3 * (groups - 1) * tokens
    text_sent = (N - 1) * text_shard + (pair - 1) * text_rows
    wait(kv_all.at[:, pl.ds(0, own_rows), :], sent.at[0])
    if bits:
        wait(kv_all.at[:, pl.ds(0, (N - 1) * shard), :], sent.at[1])
    if text_sent:
        wait(text_all.at[:, pl.ds(0, text_sent), :], sent.at[2])
    wait(so_ref, o_recv.at[0])
    wait(co_ref, o_recv.at[1])


def store(s_ref, c_ref, s_hbm, c_hbm, done):
    copies = [
        pltpu.make_async_copy(src, dst, done.at[index])
        for index, (src, dst) in enumerate(((s_ref, s_hbm), (c_ref, c_hbm)))
    ]
    for copy in copies:
        copy.start()
    for copy in copies:
        copy.wait()


def body(self_query, self_key, self_value, cross_query, text_key, text_value, padded_count):
    B = lax.axis_size("blk")
    U = lax.axis_size("uly")
    tokens, channels = self_query.shape
    group_heads = channels // HD // U
    pair = 2 if group_heads % 2 == 0 and B % 2 == 0 else 1
    heads = group_heads // pair
    N = B // pair
    width = heads * HD
    grid_width = TW * U
    shard_rows = TH * grid_width
    total = B * shard_rows
    bits = max(int(math.log2(N)), 1)
    text_total = text_key.shape[0] * B

    t, i, j = np.meshgrid(np.arange(U), np.arange(TH), np.arange(TW), indexing="ij")
    local = (i * grid_width + t * TW + j).reshape(-1)
    positions = (np.arange(B)[:, None] * shard_rows + local[None, :]).reshape(1, -1)
    perm = np.zeros((shard_rows, shard_rows), np.float32)
    perm[local, np.arange(shard_rows)] = 1.0
    spin = np.zeros((HD, HD), np.float32)
    even = np.arange(0, HD, 2)
    spin[even + 1, even] = -1.0
    spin[even, even + 1] = 1.0

    rope_blk, rope_col = rope_parts(B, U)
    gathered = sum(len(pieces(heads, cut)) for cut in (VALUE_CUT, KEY_CUT))
    parts = gathered + sum(len(pieces(heads, cut)) for cut in (CROSS_CUT, QUERY_CUT))

    vmem = pl.BlockSpec(memory_space=pltpu.VMEM)
    any_ = pl.BlockSpec(memory_space=pltpu.HBM)
    dma = pltpu.SemaphoreType.DMA
    bf = jnp.bfloat16
    chip = U * pair * tokens
    self_out, cross_out = pl.pallas_call(
        functools.partial(kernel, (U, pair, N, heads)),
        out_shape=[pltpu.VMEM((tokens, channels), bf)] * 2,
        in_specs=[pl.BlockSpec(memory_space=pltpu.SMEM), any_, any_, any_, any_, any_, any_]
        + [any_] * 5,
        out_specs=[vmem, vmem],
        scratch_shapes=[
            pltpu.VMEM((HD, HD), bf),
            pltpu.VMEM((shard_rows, shard_rows), bf),
            pltpu.VMEM((1, total), jnp.int32),
            pltpu.VMEM((tokens, channels), bf),
            pltpu.VMEM((tokens, channels), bf),
            pltpu.VMEM((tokens, channels), bf),
            pltpu.VMEM((2, tokens, 2 * HD), jnp.float32),
            pltpu.VMEM((tokens, channels), bf),
            pltpu.VMEM((tokens, channels), bf),
            pltpu.VMEM((2, total, width), bf),
            pltpu.VMEM((chip, width), bf),
            pltpu.VMEM((chip, width), bf),
            pltpu.VMEM((2, text_total, width), bf),
            pltpu.VMEM((chip, width), bf),
            pltpu.VMEM((chip, width), bf),
            pltpu.VMEM((1, total), jnp.float32),
            dma((parts,)),
            dma((bits, gathered)),
            dma,
            dma((bits,)),
            dma((2,)),
            dma((3,)),
            dma((4,)),
            pltpu.SemaphoreType.REGULAR((5,)),
        ],
        compiler_params=pltpu.CompilerParams(
            collective_id=0, has_side_effects=True, vmem_limit_bytes=67043328 - 4 * tokens * channels
        ),
    )(
        padded_count, self_query, self_key, self_value, cross_query, text_key, text_value,
        jnp.asarray(rope_blk), jnp.asarray(rope_col),
        jnp.asarray(spin, bf), jnp.asarray(perm, bf), jnp.asarray(positions, jnp.int32),
    )
    return pl.pallas_call(
        store,
        out_shape=[jax.ShapeDtypeStruct((tokens, channels), bf)] * 2,
        in_specs=[pl.BlockSpec(memory_space=pl.ANY)] * 2,
        out_specs=[any_, any_],
        scratch_shapes=[dma((2,))],
        compiler_params=pltpu.CompilerParams(vmem_limit_bytes=1 << 20),
    )(self_out, cross_out)


def solution(mesh):
    rows = P(("blk", "uly"), None)
    text = P("blk", "uly")
    return jax.shard_map(
        body,
        mesh=mesh,
        in_specs=(rows, rows, rows, rows, text, text, P()),
        out_specs=(rows, rows),
        check_vma=False,
    )
```

```python
import functools
import math

import jax
import jax.numpy as jnp
import numpy as np
from jax import lax
from jax.experimental import pallas as pl
from jax.experimental.pallas import tpu as pltpu
from jax.sharding import PartitionSpec as P

HD = 128
TH = 4
TW = 10
ROW_TILES = 8

MESH = pl.DeviceIdType.MESH
neg_fill = -1e30
KEY_BLOCK = 1280
VALUE_CUT = (1, 2, 2)
KEY_CUT = (1, 2, 2)
CROSS_CUT = (1, 4)
QUERY_CUT = (5,)
CROSS_BACK = (1,)
SELF_BACK = (1, 4)
BACK_ROUTE = ((2, 3, 1), (0, 3, 2), (0, 3, 1), (0, 1, 2))


def pieces(heads, sizes):
    cuts, start, index = [], 0, 0
    while start < heads:
        stop = min(heads, start + sizes[min(index, len(sizes) - 1)])
        cuts.append((start, stop))
        start, index = stop, index + 1
    return cuts


def rope_parts(blocks, groups):
    grid_height, grid_width = TH * ROW_TILES, TW * groups
    side = HD // 6
    first = HD // 2 - 2 * side
    pair = np.arange(HD) // 2
    start = np.where(pair < first, 0, np.where(pair < first + side, first, first + side))
    power = -((pair - start) / np.where(pair < first, first, side))
    omegas = np.power(10000.0, power).astype(np.float32)
    i, j = (axis.reshape(-1) for axis in np.meshgrid(np.arange(TH), np.arange(TW), indexing="ij"))
    rows = np.arange(blocks)[:, None] * TH + i[None, :]
    cols = np.arange(groups)[:, None] * TW + j[None, :]
    by_block = np.where(
        pair < first, (rows // grid_height)[..., None], (rows % grid_height)[..., None]
    )
    is_col = pair >= first + side

    def table(position, mine):
        angles = position.astype(np.float32) * omegas
        parts = [np.where(mine, np.cos(angles), 0), np.where(mine, np.sin(angles), 0)]
        return np.concatenate(parts, axis=-1).astype(np.float32)

    return table(by_block, ~is_col), table(np.broadcast_to(cols[..., None], cols.shape + (HD,)), is_col)


def dot(a, b):
    return jnp.dot(a, b, preferred_element_type=jnp.float32)


def dot_t(a, b):
    return lax.dot_general(a, b, (((1,), (1,)), ((), ())), preferred_element_type=jnp.float32)


def attend(queries, key_ref, value_ref, cols, bias_ref, factor):
    rows = key_ref.shape[0]
    step = rows if rows <= 2 * KEY_BLOCK else KEY_BLOCK

    def scores_of(start):
        s = dot_t(queries, key_ref[pl.ds(start, step), cols]) * factor
        if bias_ref is not None:
            s = s + bias_ref[:, pl.ds(start, step)]
        return s

    if step == rows:
        s = scores_of(0)
        w = jnp.exp2(s - jnp.max(s, axis=1, keepdims=True))
        total = jnp.sum(w, axis=1, keepdims=True)
        out = dot(w.astype(jnp.bfloat16), value_ref[:, cols])
        return (out / total).astype(jnp.bfloat16)

    def advance(index, state):
        peak, total, out = state
        start = pl.multiple_of(index * step, step)
        s = scores_of(start)
        new_peak = jnp.maximum(peak, jnp.max(s, axis=1, keepdims=True))
        w = jnp.exp2(s - new_peak)
        shrink = jnp.exp2(peak - new_peak)
        total = total * shrink + jnp.sum(w, axis=1, keepdims=True)
        out = out * shrink + dot(w.astype(jnp.bfloat16), value_ref[pl.ds(start, step), cols])
        return new_peak, total, out

    m = queries.shape[0]
    state = (
        jnp.full((m, 1), neg_fill, jnp.float32),
        jnp.zeros((m, 1), jnp.float32),
        jnp.zeros((m, HD), jnp.float32),
    )
    peak, total, out = lax.fori_loop(0, rows // step, advance, state)
    return (out / total).astype(jnp.bfloat16)


def kernel(cfg, pad_ref, q_hbm, k_hbm, v_hbm, c_ref, tk_ref, tv_ref, rope_blk, rope_col, spin_hbm,
           perm_hbm, pos_hbm, so_ref, co_ref, spin_ref, perm_ref, pos_ref, v_raw, q_raw, k_raw, tab, q_src, k_src, kv_all, q_in, c_in, text_all,
           s_out, c_out, bias, in_sem, g_recv, t_in, tg_recv, o_recv, sent, load, ready):
    U, pair, N, heads = cfg
    tokens = v_hbm.shape[0]
    width = heads * HD
    groups = U * pair
    blk = lax.axis_index("blk")
    z = lax.axis_index("uly")
    n = blk // pair
    core = blk % pair
    me = z * pair + core
    slot = (core * U + z) * tokens
    shard = groups * tokens
    text_rows = tk_ref.shape[0]
    text_shard = pair * text_rows
    bits = int(math.log2(N))
    staged = U == 4 and pair == 2
    factor = math.log2(math.e) / math.sqrt(HD)

    def apart(dz):
        if U & (U - 1):
            return (z + dz) % U
        out = 0
        for bit in range(U.bit_length() - 1):
            mine = (z // (1 << bit)) % 2
            out = out + (1 - mine if (dz >> bit) & 1 else mine) * (1 << bit)
        return out

    far_first = [*range(U // 2, U), *range(1, U // 2), 0] if U > 1 else [0]
    offsets = [(dz, dc) for dz in far_first for dc in reversed(range(pair))]

    def group_device(d):
        dz, dc = offsets[d - 1]
        to_z, to_core = apart(dz), (core + dc) % pair
        return to_z * pair + to_core, (n * pair + to_core, to_z)

    def back_device(d):
        if not staged:
            return group_device(d)
        place, side = (d - 1) // pair, (d - 1) % pair
        if place == U - 1:
            to_z, to_core = z, (core + 1 + side) % pair
        else:
            code = sum(route[place] * U**index for index, route in enumerate(BACK_ROUTE))
            to_z, to_core = (code // ((1 + 3 * (z % 2)) * (1 + 15 * (z // 2)))) % U, side
        return to_z * pair + to_core, (n * pair + to_core, to_z)

    def flip(index, bit):
        return index + (1 - 2 * ((index // (1 << bit)) % 2)) * (1 << bit)

    def neighbour(bit):
        return (flip(n, bit) * pair + core, z)

    def fetch(index, src, dst):
        copy = pltpu.make_async_copy(src, dst, load.at[index])
        copy.start()
        return copy

    v_load, k_load = fetch(0, v_hbm, v_raw), fetch(1, k_hbm, k_raw)
    fetch(2, rope_blk.at[blk], tab.at[0])
    fetch(2, rope_col.at[z], tab.at[1])
    spin_load = fetch(3, spin_hbm, spin_ref)

    k_all, v_all = kv_all.at[0], kv_all.at[1]
    tk_all, tv_all = text_all.at[0], text_all.at[1]

    barrier = pltpu.get_barrier_semaphore()
    partner = (n * pair + (core + 1) % pair, z)
    inner = (z > 0) & (z < U - 1)
    across = (blk, U - 1 - z)

    def greet(sem, device):
        pl.semaphore_signal(sem, inc=1, device_id=device, device_id_type=MESH)

    if staged:
        greet(barrier, partner)

        @pl.when((core == 0) & inner)
        def _():
            greet(barrier, across)
            pl.semaphore_wait(barrier, 2)

        @pl.when((core == 0) & jnp.logical_not(inner))
        def _():
            pl.semaphore_wait(barrier, 1)

        @pl.when(core == 1)
        def _():
            for b in range(bits):
                greet(barrier, neighbour(b))

            @pl.when(z > 0)
            def _():
                greet(barrier, (blk, z - 1))

            @pl.when(z < U - 1)
            def _():
                greet(barrier, (blk, z + 1))

            @pl.when(inner)
            def _():
                pl.semaphore_wait(barrier, 3 + bits)

            @pl.when(jnp.logical_not(inner))
            def _():
                pl.semaphore_wait(barrier, 2 + bits)
    else:
        peers = [group_device(d)[1] for d in range(1, groups)] + [neighbour(b) for b in range(bits)]
        for peer in peers:
            greet(barrier, peer)
        pl.semaphore_wait(barrier, len(peers))

    def remote(src, dst, kind, recv, device):
        pltpu.make_async_remote_copy(
            src_ref=src, dst_ref=dst, send_sem=sent.at[kind], recv_sem=recv, device_id=device,
            device_id_type=MESH,
        ).start()

    def wait(ref, sem):
        pltpu.make_async_copy(ref, ref, sem).wait()

    def head_cols(h):
        return pl.ds(h * HD, HD)

    def span(piece):
        return pl.ds(piece[0] * HD, (piece[1] - piece[0]) * HD)

    def scatter_one(src, place, sem, piece, e, device):
        cols = (piece[1] - piece[0]) * HD
        block = src.at[:, pl.ds(pl.multiple_of(e * width + piece[0] * HD, HD), cols)]
        if device is None:
            pltpu.make_async_copy(block, place, sem).start()
        else:
            remote(block, place, 0, sem, device)

    def scatter(src, dst, base, sems, cuts, early=False):
        for index, piece in enumerate(cuts):
            place = dst.at[pl.ds(pl.multiple_of(base + slot, 8), tokens), span(piece)]
            for d in range(1, groups + 1):
                e, device = group_device(d)
                if d == groups:
                    scatter_one(src, place, in_sem.at[sems + index], piece, e, None)
                elif early and offsets[d - 1] == (U - 1, 0):

                    @pl.when(jnp.logical_not(inner))
                    def _():
                        scatter_one(src, place, in_sem.at[sems + index], piece, e, device)
                else:
                    scatter_one(src, place, in_sem.at[sems + index], piece, e, device)

    def scatter_early(src, dst, base, sems, cuts):
        @pl.when(inner)
        def _():
            for index, piece in enumerate(cuts):
                place = dst.at[pl.ds(pl.multiple_of(base + slot, 8), tokens), span(piece)]
                e = (U - 1 - z) * pair + core
                scatter_one(src, place, in_sem.at[sems + index], piece, e, across)

    v_cuts, k_cuts = pieces(heads, VALUE_CUT), pieces(heads, KEY_CUT)
    c_cuts, q_cuts = pieces(heads, CROSS_CUT), pieces(heads, QUERY_CUT)
    v_sems = 0
    k_sems = v_sems + len(v_cuts)
    c_sems = k_sems + len(k_cuts)
    q_sems = c_sems + len(c_cuts)

    def gossip():
        low, high, side, far, go = (ready.at[index] for index in range(5))

        @pl.when(z > 0)
        def _():
            greet(high, (blk, z - 1))

        @pl.when(z < U - 1)
        def _():
            greet(low, (blk, z + 1))

        for b in range(bits):
            greet(side, neighbour(b))

        @pl.when(z == 1)
        def _():
            pl.semaphore_wait(low, 1)
            greet(far, (blk, 2))
            pl.semaphore_wait(high, 1)
            greet(far, (blk, 0))
            pl.semaphore_wait(far, 1)
            greet(far, (blk, 0))

        @pl.when(z == 2)
        def _():
            pl.semaphore_wait(low, 1)
            greet(far, (blk, 3))
            pl.semaphore_wait(high, 1)
            greet(far, (blk, 1))
            pl.semaphore_wait(far, 1)
            greet(far, (blk, 3))

        @pl.when(z == 0)
        def _():
            pl.semaphore_wait(high, 1)
            pl.semaphore_wait(far, 2)

        @pl.when(z == 3)
        def _():
            pl.semaphore_wait(low, 1)
            pl.semaphore_wait(far, 2)

        pl.semaphore_wait(side, bits)
        greet(go, partner)

    def shard_at(ref, index, rows, cols):
        return ref.at[pl.ds(pl.multiple_of(index * rows, 8), rows), cols]

    def held(order, stage):
        lists = [[n]]
        for s in range(stage):
            lists.append([flip(i, order[s]) for part in lists for i in part])
        return lists

    def gather_send(ref, rows, cols, order, arrived, kind, recv_at):
        for stage in range(arrived, bits):
            device = neighbour(order[stage])
            for index in held(order, arrived)[arrived]:
                block = shard_at(ref, index, rows, cols)
                remote(block, block, kind, recv_at(stage), device)

    def gather_wait(ref, rows, cols, stage, recv_at):
        wait(ref.at[pl.ds(0, rows << stage), cols], recv_at(stage))

    orders = [list(range(bits)), list(range(bits))[::-1]]
    everything = pl.ds(0, width)

    def rope(src, dst):
        cos = tab[0, :, 0:HD] + tab[1, :, 0:HD]
        sin = tab[0, :, HD:] + tab[1, :, HD:]
        for g in range(src.shape[1] // HD):
            x = src[:, head_cols(g)]
            turned = x.astype(jnp.float32) * cos + dot(x, spin_ref[...]) * sin
            dst[:, head_cols(g)] = turned.astype(jnp.bfloat16)

    values_out = (v_raw, v_all, n * shard, v_sems, v_cuts)
    keys_out = (k_src, k_all, n * shard, k_sems, k_cuts)
    cross_out = (c_ref, c_in, 0, c_sems, c_cuts)
    v_load.wait()
    q_load = fetch(0, q_hbm, q_raw)
    if staged:
        scatter_early(*values_out)
        scatter_early(*cross_out)

        @pl.when(core == 1)
        def _():
            gossip()
            scatter(*values_out, True)

    k_load.wait()
    wait(tab, load.at[2])
    spin_load.wait()
    perm_load, pos_load = fetch(1, perm_hbm, perm_ref), fetch(3, pos_hbm, pos_ref)
    rope(k_raw, k_src)
    if staged:

        @pl.when(core == 0)
        def _():
            pl.semaphore_wait(ready.at[4], 1)
            scatter(*values_out, True)
    else:
        scatter(*values_out)

    text = ((tk_ref, tk_all, 0), (tv_ref, tv_all, 1))
    for src, dst, a in text:
        for d in range(pair):
            k = (core + d) % pair
            block = src.at[:, pl.ds(pl.multiple_of(k * width, HD), width)]
            place = dst.at[
                pl.ds(pl.multiple_of(n * text_shard + core * text_rows, 8), text_rows), everything
            ]
            if d == 0:
                pltpu.make_async_copy(block, place, t_in).start()
            else:
                remote(block, place, 2, t_in, (n * pair + k, z))

    scatter(*keys_out)
    scatter(*cross_out, staged)
    perm_load.wait()
    pos_load.wait()
    bias[...] = jnp.where(pos_ref[...] < k_all.shape[0] - pad_ref[0], 0.0, neg_fill)

    def text_recv(stage):
        return tg_recv.at[stage]

    def text_wait(stage):
        wait(text_all.at[:, pl.ds(0, text_shard << stage), :], tg_recv.at[stage])

    wait(text_all.at[:, pl.ds(0, text_shard), :], t_in)
    for _, dst, a in text:
        gather_send(dst, text_shard, everything, orders[a], 0, 2, text_recv)
    keys, values = (k_all, k_sems, 0, k_cuts), (v_all, v_sems, 1, v_cuts)

    def main_recv(sems, index):
        return lambda stage: g_recv.at[stage, sems + index]

    def own_sends(array, index):
        ref, sems, a, cuts = array
        cols = span(cuts[index])
        wait(shard_at(ref, n, shard, cols), in_sem.at[sems + index])
        gather_send(ref, shard, cols, orders[a], 0, 1, main_recv(sems, index))

    def relay(array, index):
        ref, sems, a, cuts = array
        cols = span(cuts[index])
        for stage in range(bits - 1):
            gather_wait(ref, shard, cols, stage, main_recv(sems, index))
            gather_send(ref, shard, cols, orders[a], stage + 1, 1, main_recv(sems, index))

    def settle(array, index):
        ref, sems, a, cuts = array
        if bits:
            gather_wait(ref, shard, span(cuts[index]), bits - 1, main_recv(sems, index))

    def opens(cuts, h):
        return [index for index, piece in enumerate(cuts) if piece[0] == h]

    def run_head(q_ref, key_ref, value_ref, bias_ref, out_ref, h):
        part = U * tokens

        for index in range(pair):
            rows = pl.ds(index * part, part)
            ordered = dot(perm_ref[...], q_ref[rows, head_cols(h)]).astype(jnp.bfloat16)
            out_ref[rows, head_cols(h)] = attend(
                ordered, key_ref, value_ref, head_cols(h), bias_ref, factor
            )

    def give_back(src, dst, recv, cuts, h):
        for piece in cuts:
            if piece[1] != h + 1:
                continue
            cols = (piece[1] - piece[0]) * HD
            for d in range(1, groups + 1):
                device = back_device(d)[1]
                row = (device[0] % pair * U + device[1]) * tokens
                block = src.at[pl.ds(pl.multiple_of(row, 8), tokens), span(piece)]
                place = dst.at[:, pl.ds(pl.multiple_of(me * width + piece[0] * HD, HD), cols)]
                if d == groups:
                    pltpu.make_async_copy(block, place, recv).start()
                else:
                    remote(block, place, 0, recv, device)

    for index in range(len(v_cuts)):
        own_sends(values, index)
    q_load.wait()
    rope(q_raw, q_src)
    scatter(q_src, q_in, 0, q_sems, q_cuts)
    for stage in range(bits - 1):
        text_wait(stage)
        for _, dst, a in text:
            gather_send(dst, text_shard, everything, orders[a], stage + 1, 2, text_recv)
    for index in range(len(k_cuts)):
        own_sends(keys, index)
        if 0 < index <= len(v_cuts):
            relay(values, index - 1)
    for index in range(len(k_cuts) - 1, len(v_cuts)):
        relay(values, index)
    if bits:
        text_wait(bits - 1)
    c_back, s_back = pieces(heads, CROSS_BACK), pieces(heads, SELF_BACK)
    for h in range(heads):
        for index in opens(k_cuts, h):
            relay(keys, index)
        for index in opens(c_cuts, h):
            wait(c_in.at[:, span(c_cuts[index])], in_sem.at[c_sems + index])
        run_head(c_in, tk_all, tv_all, None, c_out, h)
        give_back(c_out, co_ref, o_recv.at[1], c_back, h)
    for h in range(heads):
        for index in opens(q_cuts, h):
            wait(q_in.at[:, span(q_cuts[index])], in_sem.at[q_sems + index])
        for index in opens(v_cuts, h):
            settle(values, index)
        for index in opens(k_cuts, h):
            settle(keys, index)
        run_head(q_in, k_all, v_all, bias, s_out, h)
        give_back(s_out, so_ref, o_recv.at[0], s_back, h)

    own_rows = 3 * (groups - 1) * tokens
    text_sent = (N - 1) * text_shard + (pair - 1) * text_rows
    wait(kv_all.at[:, pl.ds(0, own_rows), :], sent.at[0])
    if bits:
        wait(kv_all.at[:, pl.ds(0, (N - 1) * shard), :], sent.at[1])
    if text_sent:
        wait(text_all.at[:, pl.ds(0, text_sent), :], sent.at[2])
    wait(so_ref, o_recv.at[0])
    wait(co_ref, o_recv.at[1])


def store(s_ref, c_ref, s_hbm, c_hbm, done):
    copies = [
        pltpu.make_async_copy(src, dst, done.at[index])
        for index, (src, dst) in enumerate(((s_ref, s_hbm), (c_ref, c_hbm)))
    ]
    for copy in copies:
        copy.start()
    for copy in copies:
        copy.wait()


def body(self_query, self_key, self_value, cross_query, text_key, text_value, padded_count):
    B = lax.axis_size("blk")
    U = lax.axis_size("uly")
    tokens, channels = self_query.shape
    group_heads = channels // HD // U
    pair = 2 if group_heads % 2 == 0 and B % 2 == 0 else 1
    heads = group_heads // pair
    N = B // pair
    width = heads * HD
    grid_width = TW * U
    shard_rows = TH * grid_width
    total = B * shard_rows
    bits = max(int(math.log2(N)), 1)
    text_total = text_key.shape[0] * B

    t, i, j = np.meshgrid(np.arange(U), np.arange(TH), np.arange(TW), indexing="ij")
    local = (i * grid_width + t * TW + j).reshape(-1)
    positions = (np.arange(B)[:, None] * shard_rows + local[None, :]).reshape(1, -1)
    perm = np.zeros((shard_rows, shard_rows), np.float32)
    perm[local, np.arange(shard_rows)] = 1.0
    spin = np.zeros((HD, HD), np.float32)
    even = np.arange(0, HD, 2)
    spin[even + 1, even] = -1.0
    spin[even, even + 1] = 1.0

    rope_blk, rope_col = rope_parts(B, U)
    gathered = sum(len(pieces(heads, cut)) for cut in (VALUE_CUT, KEY_CUT))
    parts = gathered + sum(len(pieces(heads, cut)) for cut in (CROSS_CUT, QUERY_CUT))

    vmem = pl.BlockSpec(memory_space=pltpu.VMEM)
    any_ = pl.BlockSpec(memory_space=pltpu.HBM)
    dma = pltpu.SemaphoreType.DMA
    bf = jnp.bfloat16
    chip = U * pair * tokens
    self_out, cross_out = pl.pallas_call(
        functools.partial(kernel, (U, pair, N, heads)),
        out_shape=[pltpu.VMEM((tokens, channels), bf)] * 2,
        in_specs=[pl.BlockSpec(memory_space=pltpu.SMEM), any_, any_, any_, any_, any_, any_]
        + [any_] * 5,
        out_specs=[vmem, vmem],
        scratch_shapes=[
            pltpu.VMEM((HD, HD), bf),
            pltpu.VMEM((shard_rows, shard_rows), bf),
            pltpu.VMEM((1, total), jnp.int32),
            pltpu.VMEM((tokens, channels), bf),
            pltpu.VMEM((tokens, channels), bf),
            pltpu.VMEM((tokens, channels), bf),
            pltpu.VMEM((2, tokens, 2 * HD), jnp.float32),
            pltpu.VMEM((tokens, channels), bf),
            pltpu.VMEM((tokens, channels), bf),
            pltpu.VMEM((2, total, width), bf),
            pltpu.VMEM((chip, width), bf),
            pltpu.VMEM((chip, width), bf),
            pltpu.VMEM((2, text_total, width), bf),
            pltpu.VMEM((chip, width), bf),
            pltpu.VMEM((chip, width), bf),
            pltpu.VMEM((1, total), jnp.float32),
            dma((parts,)),
            dma((bits, gathered)),
            dma,
            dma((bits,)),
            dma((2,)),
            dma((3,)),
            dma((4,)),
            pltpu.SemaphoreType.REGULAR((5,)),
        ],
        compiler_params=pltpu.CompilerParams(
            collective_id=0, has_side_effects=True, vmem_limit_bytes=67043328 - 4 * tokens * channels
        ),
    )(
        padded_count, self_query, self_key, self_value, cross_query, text_key, text_value,
        jnp.asarray(rope_blk), jnp.asarray(rope_col),
        jnp.asarray(spin, bf), jnp.asarray(perm, bf), jnp.asarray(positions, jnp.int32),
    )
    return pl.pallas_call(
        store,
        out_shape=[jax.ShapeDtypeStruct((tokens, channels), bf)] * 2,
        in_specs=[pl.BlockSpec(memory_space=pl.ANY)] * 2,
        out_specs=[any_, any_],
        scratch_shapes=[dma((2,))],
        compiler_params=pltpu.CompilerParams(vmem_limit_bytes=1 << 20),
    )(self_out, cross_out)


def solution(mesh):
    rows = P(("blk", "uly"), None)
    text = P("blk", "uly")
    return jax.shard_map(
        body,
        mesh=mesh,
        in_specs=(rows, rows, rows, rows, text, text, P()),
        out_specs=(rows, rows),
        check_vma=False,
    )
```

```python
import functools
import math

import jax
import jax.numpy as jnp
import numpy as np
from jax import lax
from jax.experimental import pallas as pl
from jax.experimental.pallas import tpu as pltpu
from jax.sharding import PartitionSpec as P

HD = 128
TH = 4
TW = 10
ROW_TILES = 8

MESH = pl.DeviceIdType.MESH
neg_fill = -1e30
KEY_BLOCK = 1280
VALUE_CUT = (1, 2, 2)
KEY_CUT = (1, 2, 2)
CROSS_CUT = (1, 4)
QUERY_CUT = (5,)
CROSS_BACK = (1,)
SELF_BACK = (1, 4)
BACK_ROUTE = ((2, 3, 1), (0, 3, 2), (0, 3, 1), (0, 1, 2))


def pieces(heads, sizes):
    cuts, start, index = [], 0, 0
    while start < heads:
        stop = min(heads, start + sizes[min(index, len(sizes) - 1)])
        cuts.append((start, stop))
        start, index = stop, index + 1
    return cuts


def rope_parts(blocks, groups):
    grid_height, grid_width = TH * ROW_TILES, TW * groups
    side = HD // 6
    first = HD // 2 - 2 * side
    pair = np.arange(HD) // 2
    start = np.where(pair < first, 0, np.where(pair < first + side, first, first + side))
    power = -((pair - start) / np.where(pair < first, first, side))
    omegas = np.power(10000.0, power).astype(np.float32)
    i, j = (axis.reshape(-1) for axis in np.meshgrid(np.arange(TH), np.arange(TW), indexing="ij"))
    rows = np.arange(blocks)[:, None] * TH + i[None, :]
    cols = np.arange(groups)[:, None] * TW + j[None, :]
    by_block = np.where(
        pair < first, (rows // grid_height)[..., None], (rows % grid_height)[..., None]
    )
    is_col = pair >= first + side

    def table(position, mine):
        angles = position.astype(np.float32) * omegas
        parts = [np.where(mine, np.cos(angles), 0), np.where(mine, np.sin(angles), 0)]
        return np.concatenate(parts, axis=-1).astype(np.float32)

    return table(by_block, ~is_col), table(np.broadcast_to(cols[..., None], cols.shape + (HD,)), is_col)


def dot(a, b):
    return jnp.dot(a, b, preferred_element_type=jnp.float32)


def dot_t(a, b):
    return lax.dot_general(a, b, (((1,), (1,)), ((), ())), preferred_element_type=jnp.float32)


def attend(queries, key_ref, value_ref, cols, bias_ref, factor):
    rows = key_ref.shape[0]
    step = rows if rows <= 2 * KEY_BLOCK else KEY_BLOCK

    def scores_of(start):
        s = dot_t(queries, key_ref[pl.ds(start, step), cols]) * factor
        if bias_ref is not None:
            s = s + bias_ref[:, pl.ds(start, step)]
        return s

    if step == rows:
        s = scores_of(0)
        w = jnp.exp2(s - jnp.max(s, axis=1, keepdims=True))
        total = jnp.sum(w, axis=1, keepdims=True)
        out = dot(w.astype(jnp.bfloat16), value_ref[:, cols])
        return (out / total).astype(jnp.bfloat16)

    def advance(index, state):
        peak, total, out = state
        start = pl.multiple_of(index * step, step)
        s = scores_of(start)
        new_peak = jnp.maximum(peak, jnp.max(s, axis=1, keepdims=True))
        w = jnp.exp2(s - new_peak)
        shrink = jnp.exp2(peak - new_peak)
        total = total * shrink + jnp.sum(w, axis=1, keepdims=True)
        out = out * shrink + dot(w.astype(jnp.bfloat16), value_ref[pl.ds(start, step), cols])
        return new_peak, total, out

    m = queries.shape[0]
    state = (
        jnp.full((m, 1), neg_fill, jnp.float32),
        jnp.zeros((m, 1), jnp.float32),
        jnp.zeros((m, HD), jnp.float32),
    )
    peak, total, out = lax.fori_loop(0, rows // step, advance, state)
    return (out / total).astype(jnp.bfloat16)


def kernel(cfg, pad_ref, q_hbm, k_hbm, v_hbm, c_ref, tk_ref, tv_ref, rope_blk, rope_col, spin_hbm,
           perm_hbm, pos_hbm, so_ref, co_ref, spin_ref, perm_ref, pos_ref, v_raw, q_raw, k_raw, tab, q_src, k_src, kv_all, q_in, c_in, text_all,
           s_out, c_out, bias, in_sem, g_recv, t_in, tg_recv, o_recv, sent, load, ready):
    U, pair, N, heads = cfg
    tokens = v_hbm.shape[0]
    width = heads * HD
    groups = U * pair
    blk = lax.axis_index("blk")
    z = lax.axis_index("uly")
    n = blk // pair
    core = blk % pair
    me = z * pair + core
    slot = (core * U + z) * tokens
    shard = groups * tokens
    text_rows = tk_ref.shape[0]
    text_shard = pair * text_rows
    bits = int(math.log2(N))
    staged = U == 4 and pair == 2
    factor = math.log2(math.e) / math.sqrt(HD)

    def apart(dz):
        if U & (U - 1):
            return (z + dz) % U
        out = 0
        for bit in range(U.bit_length() - 1):
            mine = (z // (1 << bit)) % 2
            out = out + (1 - mine if (dz >> bit) & 1 else mine) * (1 << bit)
        return out

    far_first = [*range(U // 2, U), *range(1, U // 2), 0] if U > 1 else [0]
    offsets = [(dz, dc) for dz in far_first for dc in reversed(range(pair))]

    def group_device(d):
        dz, dc = offsets[d - 1]
        to_z, to_core = apart(dz), (core + dc) % pair
        return to_z * pair + to_core, (n * pair + to_core, to_z)

    def back_device(d):
        if not staged:
            return group_device(d)
        place, side = (d - 1) // pair, (d - 1) % pair
        if place == U - 1:
            to_z, to_core = z, (core + 1 + side) % pair
        else:
            code = sum(route[place] * U**index for index, route in enumerate(BACK_ROUTE))
            to_z, to_core = (code // ((1 + 3 * (z % 2)) * (1 + 15 * (z // 2)))) % U, side
        return to_z * pair + to_core, (n * pair + to_core, to_z)

    def flip(index, bit):
        return index + (1 - 2 * ((index // (1 << bit)) % 2)) * (1 << bit)

    def neighbour(bit):
        return (flip(n, bit) * pair + core, z)

    def fetch(index, src, dst):
        copy = pltpu.make_async_copy(src, dst, load.at[index])
        copy.start()
        return copy

    v_load, k_load = fetch(0, v_hbm, v_raw), fetch(1, k_hbm, k_raw)
    fetch(2, rope_blk.at[blk], tab.at[0])
    fetch(2, rope_col.at[z], tab.at[1])
    spin_load = fetch(3, spin_hbm, spin_ref)

    k_all, v_all = kv_all.at[0], kv_all.at[1]
    tk_all, tv_all = text_all.at[0], text_all.at[1]

    barrier = pltpu.get_barrier_semaphore()
    partner = (n * pair + (core + 1) % pair, z)
    inner = (z > 0) & (z < U - 1)
    across = (blk, U - 1 - z)

    def greet(sem, device):
        pl.semaphore_signal(sem, inc=1, device_id=device, device_id_type=MESH)

    if staged:
        greet(barrier, partner)

        @pl.when((core == 0) & inner)
        def _():
            greet(barrier, across)
            pl.semaphore_wait(barrier, 2)

        @pl.when((core == 0) & jnp.logical_not(inner))
        def _():
            pl.semaphore_wait(barrier, 1)

        @pl.when(core == 1)
        def _():
            for b in range(bits):
                greet(barrier, neighbour(b))

            @pl.when(z > 0)
            def _():
                greet(barrier, (blk, z - 1))

            @pl.when(z < U - 1)
            def _():
                greet(barrier, (blk, z + 1))

            @pl.when(inner)
            def _():
                pl.semaphore_wait(barrier, 3 + bits)

            @pl.when(jnp.logical_not(inner))
            def _():
                pl.semaphore_wait(barrier, 2 + bits)
    else:
        peers = [group_device(d)[1] for d in range(1, groups)] + [neighbour(b) for b in range(bits)]
        for peer in peers:
            greet(barrier, peer)
        pl.semaphore_wait(barrier, len(peers))

    def remote(src, dst, kind, recv, device):
        pltpu.make_async_remote_copy(
            src_ref=src, dst_ref=dst, send_sem=sent.at[kind], recv_sem=recv, device_id=device,
            device_id_type=MESH,
        ).start()

    def wait(ref, sem):
        pltpu.make_async_copy(ref, ref, sem).wait()

    def head_cols(h):
        return pl.ds(h * HD, HD)

    def span(piece):
        return pl.ds(piece[0] * HD, (piece[1] - piece[0]) * HD)

    def scatter_one(src, place, sem, piece, e, device):
        cols = (piece[1] - piece[0]) * HD
        block = src.at[:, pl.ds(pl.multiple_of(e * width + piece[0] * HD, HD), cols)]
        if device is None:
            pltpu.make_async_copy(block, place, sem).start()
        else:
            remote(block, place, 0, sem, device)

    def scatter(src, dst, base, sems, cuts, early=False):
        for index, piece in enumerate(cuts):
            place = dst.at[pl.ds(pl.multiple_of(base + slot, 8), tokens), span(piece)]
            for d in range(1, groups + 1):
                e, device = group_device(d)
                if d == groups:
                    scatter_one(src, place, in_sem.at[sems + index], piece, e, None)
                elif early and offsets[d - 1] == (U - 1, 0):

                    @pl.when(jnp.logical_not(inner))
                    def _():
                        scatter_one(src, place, in_sem.at[sems + index], piece, e, device)
                else:
                    scatter_one(src, place, in_sem.at[sems + index], piece, e, device)

    def scatter_early(src, dst, base, sems, cuts):
        @pl.when(inner)
        def _():
            for index, piece in enumerate(cuts):
                place = dst.at[pl.ds(pl.multiple_of(base + slot, 8), tokens), span(piece)]
                e = (U - 1 - z) * pair + core
                scatter_one(src, place, in_sem.at[sems + index], piece, e, across)

    v_cuts, k_cuts = pieces(heads, VALUE_CUT), pieces(heads, KEY_CUT)
    c_cuts, q_cuts = pieces(heads, CROSS_CUT), pieces(heads, QUERY_CUT)
    v_sems = 0
    k_sems = v_sems + len(v_cuts)
    c_sems = k_sems + len(k_cuts)
    q_sems = c_sems + len(c_cuts)

    def gossip():
        low, high, side, far, go = (ready.at[index] for index in range(5))

        @pl.when(z > 0)
        def _():
            greet(high, (blk, z - 1))

        @pl.when(z < U - 1)
        def _():
            greet(low, (blk, z + 1))

        for b in range(bits):
            greet(side, neighbour(b))

        @pl.when(z == 1)
        def _():
            pl.semaphore_wait(low, 1)
            greet(far, (blk, 2))
            pl.semaphore_wait(high, 1)
            greet(far, (blk, 0))
            pl.semaphore_wait(far, 1)
            greet(far, (blk, 0))

        @pl.when(z == 2)
        def _():
            pl.semaphore_wait(low, 1)
            greet(far, (blk, 3))
            pl.semaphore_wait(high, 1)
            greet(far, (blk, 1))
            pl.semaphore_wait(far, 1)
            greet(far, (blk, 3))

        @pl.when(z == 0)
        def _():
            pl.semaphore_wait(high, 1)
            pl.semaphore_wait(far, 2)

        @pl.when(z == 3)
        def _():
            pl.semaphore_wait(low, 1)
            pl.semaphore_wait(far, 2)

        pl.semaphore_wait(side, bits)
        greet(go, partner)

    def shard_at(ref, index, rows, cols):
        return ref.at[pl.ds(pl.multiple_of(index * rows, 8), rows), cols]

    def held(order, stage):
        lists = [[n]]
        for s in range(stage):
            lists.append([flip(i, order[s]) for part in lists for i in part])
        return lists

    def gather_send(ref, rows, cols, order, arrived, kind, recv_at):
        for stage in range(arrived, bits):
            device = neighbour(order[stage])
            for index in held(order, arrived)[arrived]:
                block = shard_at(ref, index, rows, cols)
                remote(block, block, kind, recv_at(stage), device)

    def gather_wait(ref, rows, cols, stage, recv_at):
        wait(ref.at[pl.ds(0, rows << stage), cols], recv_at(stage))

    orders = [list(range(bits)), list(range(bits))[::-1]]
    everything = pl.ds(0, width)

    def rope(src, dst):
        cos = tab[0, :, 0:HD] + tab[1, :, 0:HD]
        sin = tab[0, :, HD:] + tab[1, :, HD:]
        for g in range(src.shape[1] // HD):
            x = src[:, head_cols(g)]
            turned = x.astype(jnp.float32) * cos + dot(x, spin_ref[...]) * sin
            dst[:, head_cols(g)] = turned.astype(jnp.bfloat16)

    values_out = (v_raw, v_all, n * shard, v_sems, v_cuts)
    keys_out = (k_src, k_all, n * shard, k_sems, k_cuts)
    cross_out = (c_ref, c_in, 0, c_sems, c_cuts)
    v_load.wait()
    q_load = fetch(0, q_hbm, q_raw)
    if staged:
        scatter_early(*values_out)
        scatter_early(*cross_out)

        @pl.when(core == 1)
        def _():
            gossip()
            scatter(*values_out, True)

    k_load.wait()
    wait(tab, load.at[2])
    spin_load.wait()
    perm_load, pos_load = fetch(1, perm_hbm, perm_ref), fetch(3, pos_hbm, pos_ref)
    rope(k_raw, k_src)
    if staged:

        @pl.when(core == 0)
        def _():
            pl.semaphore_wait(ready.at[4], 1)
            scatter(*values_out, True)
    else:
        scatter(*values_out)

    text = ((tk_ref, tk_all, 0), (tv_ref, tv_all, 1))
    for src, dst, a in text:
        for d in range(pair):
            k = (core + d) % pair
            block = src.at[:, pl.ds(pl.multiple_of(k * width, HD), width)]
            place = dst.at[
                pl.ds(pl.multiple_of(n * text_shard + core * text_rows, 8), text_rows), everything
            ]
            if d == 0:
                pltpu.make_async_copy(block, place, t_in).start()
            else:
                remote(block, place, 2, t_in, (n * pair + k, z))

    scatter(*keys_out)
    perm_load.wait()
    pos_load.wait()
    bias[...] = jnp.where(pos_ref[...] < k_all.shape[0] - pad_ref[0], 0.0, neg_fill)

    def text_recv(stage):
        return tg_recv.at[stage]

    def text_wait(stage):
        wait(text_all.at[:, pl.ds(0, text_shard << stage), :], tg_recv.at[stage])

    wait(text_all.at[:, pl.ds(0, text_shard), :], t_in)
    for _, dst, a in text:
        gather_send(dst, text_shard, everything, orders[a], 0, 2, text_recv)
    keys, values = (k_all, k_sems, 0, k_cuts), (v_all, v_sems, 1, v_cuts)

    def main_recv(sems, index):
        return lambda stage: g_recv.at[stage, sems + index]

    def own_sends(array, index):
        ref, sems, a, cuts = array
        cols = span(cuts[index])
        wait(shard_at(ref, n, shard, cols), in_sem.at[sems + index])
        gather_send(ref, shard, cols, orders[a], 0, 1, main_recv(sems, index))

    def relay(array, index):
        ref, sems, a, cuts = array
        cols = span(cuts[index])
        for stage in range(bits - 1):
            gather_wait(ref, shard, cols, stage, main_recv(sems, index))
            gather_send(ref, shard, cols, orders[a], stage + 1, 1, main_recv(sems, index))

    def settle(array, index):
        ref, sems, a, cuts = array
        if bits:
            gather_wait(ref, shard, span(cuts[index]), bits - 1, main_recv(sems, index))

    def opens(cuts, h):
        return [index for index, piece in enumerate(cuts) if piece[0] == h]

    def run_head(q_ref, key_ref, value_ref, bias_ref, out_ref, h):
        part = U * tokens

        for index in range(pair):
            rows = pl.ds(index * part, part)
            ordered = dot(perm_ref[...], q_ref[rows, head_cols(h)]).astype(jnp.bfloat16)
            out_ref[rows, head_cols(h)] = attend(
                ordered, key_ref, value_ref, head_cols(h), bias_ref, factor
            )

    def give_back(src, dst, recv, cuts, h):
        for piece in cuts:
            if piece[1] != h + 1:
                continue
            cols = (piece[1] - piece[0]) * HD
            for d in range(1, groups + 1):
                device = back_device(d)[1]
                row = (device[0] % pair * U + device[1]) * tokens
                block = src.at[pl.ds(pl.multiple_of(row, 8), tokens), span(piece)]
                place = dst.at[:, pl.ds(pl.multiple_of(me * width + piece[0] * HD, HD), cols)]
                if d == groups:
                    pltpu.make_async_copy(block, place, recv).start()
                else:
                    remote(block, place, 0, recv, device)

    for index in range(len(v_cuts)):
        own_sends(values, index)
    scatter(*cross_out, staged)
    for stage in range(bits - 1):
        text_wait(stage)
        for _, dst, a in text:
            gather_send(dst, text_shard, everything, orders[a], stage + 1, 2, text_recv)
    for index in range(len(k_cuts)):
        own_sends(keys, index)
        if 0 < index <= len(v_cuts):
            relay(values, index - 1)
    q_load.wait()
    rope(q_raw, q_src)
    scatter(q_src, q_in, 0, q_sems, q_cuts)
    for index in range(len(k_cuts) - 1, len(v_cuts)):
        relay(values, index)
    if bits:
        text_wait(bits - 1)
    c_back, s_back = pieces(heads, CROSS_BACK), pieces(heads, SELF_BACK)
    for h in range(heads):
        for index in opens(k_cuts, h):
            relay(keys, index)
        for index in opens(c_cuts, h):
            wait(c_in.at[:, span(c_cuts[index])], in_sem.at[c_sems + index])
        run_head(c_in, tk_all, tv_all, None, c_out, h)
        give_back(c_out, co_ref, o_recv.at[1], c_back, h)
    for h in range(heads):
        for index in opens(q_cuts, h):
            wait(q_in.at[:, span(q_cuts[index])], in_sem.at[q_sems + index])
        for index in opens(v_cuts, h):
            settle(values, index)
        for index in opens(k_cuts, h):
            settle(keys, index)
        run_head(q_in, k_all, v_all, bias, s_out, h)
        give_back(s_out, so_ref, o_recv.at[0], s_back, h)

    own_rows = 3 * (groups - 1) * tokens
    text_sent = (N - 1) * text_shard + (pair - 1) * text_rows
    wait(kv_all.at[:, pl.ds(0, own_rows), :], sent.at[0])
    if bits:
        wait(kv_all.at[:, pl.ds(0, (N - 1) * shard), :], sent.at[1])
    if text_sent:
        wait(text_all.at[:, pl.ds(0, text_sent), :], sent.at[2])
    wait(so_ref, o_recv.at[0])
    wait(co_ref, o_recv.at[1])


def store(s_ref, c_ref, s_hbm, c_hbm, done):
    copies = [
        pltpu.make_async_copy(src, dst, done.at[index])
        for index, (src, dst) in enumerate(((s_ref, s_hbm), (c_ref, c_hbm)))
    ]
    for copy in copies:
        copy.start()
    for copy in copies:
        copy.wait()


def body(self_query, self_key, self_value, cross_query, text_key, text_value, padded_count):
    B = lax.axis_size("blk")
    U = lax.axis_size("uly")
    tokens, channels = self_query.shape
    group_heads = channels // HD // U
    pair = 2 if group_heads % 2 == 0 and B % 2 == 0 else 1
    heads = group_heads // pair
    N = B // pair
    width = heads * HD
    grid_width = TW * U
    shard_rows = TH * grid_width
    total = B * shard_rows
    bits = max(int(math.log2(N)), 1)
    text_total = text_key.shape[0] * B

    t, i, j = np.meshgrid(np.arange(U), np.arange(TH), np.arange(TW), indexing="ij")
    local = (i * grid_width + t * TW + j).reshape(-1)
    positions = (np.arange(B)[:, None] * shard_rows + local[None, :]).reshape(1, -1)
    perm = np.zeros((shard_rows, shard_rows), np.float32)
    perm[local, np.arange(shard_rows)] = 1.0
    spin = np.zeros((HD, HD), np.float32)
    even = np.arange(0, HD, 2)
    spin[even + 1, even] = -1.0
    spin[even, even + 1] = 1.0

    rope_blk, rope_col = rope_parts(B, U)
    gathered = sum(len(pieces(heads, cut)) for cut in (VALUE_CUT, KEY_CUT))
    parts = gathered + sum(len(pieces(heads, cut)) for cut in (CROSS_CUT, QUERY_CUT))

    vmem = pl.BlockSpec(memory_space=pltpu.VMEM)
    any_ = pl.BlockSpec(memory_space=pltpu.HBM)
    dma = pltpu.SemaphoreType.DMA
    bf = jnp.bfloat16
    chip = U * pair * tokens
    self_out, cross_out = pl.pallas_call(
        functools.partial(kernel, (U, pair, N, heads)),
        out_shape=[pltpu.VMEM((tokens, channels), bf)] * 2,
        in_specs=[pl.BlockSpec(memory_space=pltpu.SMEM), any_, any_, any_, any_, any_, any_]
        + [any_] * 5,
        out_specs=[vmem, vmem],
        scratch_shapes=[
            pltpu.VMEM((HD, HD), bf),
            pltpu.VMEM((shard_rows, shard_rows), bf),
            pltpu.VMEM((1, total), jnp.int32),
            pltpu.VMEM((tokens, channels), bf),
            pltpu.VMEM((tokens, channels), bf),
            pltpu.VMEM((tokens, channels), bf),
            pltpu.VMEM((2, tokens, 2 * HD), jnp.float32),
            pltpu.VMEM((tokens, channels), bf),
            pltpu.VMEM((tokens, channels), bf),
            pltpu.VMEM((2, total, width), bf),
            pltpu.VMEM((chip, width), bf),
            pltpu.VMEM((chip, width), bf),
            pltpu.VMEM((2, text_total, width), bf),
            pltpu.VMEM((chip, width), bf),
            pltpu.VMEM((chip, width), bf),
            pltpu.VMEM((1, total), jnp.float32),
            dma((parts,)),
            dma((bits, gathered)),
            dma,
            dma((bits,)),
            dma((2,)),
            dma((3,)),
            dma((4,)),
            pltpu.SemaphoreType.REGULAR((5,)),
        ],
        compiler_params=pltpu.CompilerParams(
            collective_id=0, has_side_effects=True, vmem_limit_bytes=67043328 - 4 * tokens * channels
        ),
    )(
        padded_count, self_query, self_key, self_value, cross_query, text_key, text_value,
        jnp.asarray(rope_blk), jnp.asarray(rope_col),
        jnp.asarray(spin, bf), jnp.asarray(perm, bf), jnp.asarray(positions, jnp.int32),
    )
    return pl.pallas_call(
        store,
        out_shape=[jax.ShapeDtypeStruct((tokens, channels), bf)] * 2,
        in_specs=[pl.BlockSpec(memory_space=pl.ANY)] * 2,
        out_specs=[any_, any_],
        scratch_shapes=[dma((2,))],
        compiler_params=pltpu.CompilerParams(vmem_limit_bytes=1 << 20),
    )(self_out, cross_out)


def solution(mesh):
    rows = P(("blk", "uly"), None)
    text = P("blk", "uly")
    return jax.shard_map(
        body,
        mesh=mesh,
        in_specs=(rows, rows, rows, rows, text, text, P()),
        out_specs=(rows, rows),
        check_vma=False,
    )
```
